32 devices in a mesh: front: 8 (over y, x, core), sub: 4 (over z).
Axes of the slice: x: 2, y: 2, z: 4, core: 2. Of those that a mesh axis runs over, the one named last changes fastest.
Arguments:
- row_values: float32 [4096, 1024], P(('front', 'sub')), may hold values from -0.12 to 0.12
- front_of_row: int32 [4096, 1], P(('front', 'sub')), may hold values from 0 to 7; in each aligned block of 128 rows (0 to 127, 128 to 255, ...) at most 32 rows name the same one
- child_factors: float32 [16, 512, 512], P('front', 'sub'), as said below
- child_columns: int32 [16, 512], P('front'), may hold values from 0 to 1023, as said below
- damping: float32 [8, 1024], P('front'), may hold values from 0.5 to 2
Outputs:
- front_factor: float32 [8, 1024, 1024], P('front', 'sub')
The draws below stay inside these ranges and needn't reach their ends.
Inputs may be any that keep to these rules, and one draw needn't show every extreme that they name: `front_of_row`: among the 128 rows of one device, at most 32 name the same front, and some device's block reaches this bound. `child_factors`: each block is upper triangular with a positive diagonal. `child_columns`: each row names 512 distinct columns.
All inputs are finite; a program needn't handle non-finite values.
Results may differ from the reference program's by a relative error of at most 0.0003.
Values sent between devices are 32-bit elements; how exact they have to be, the bound alone decides.
A program may use at most 64 MiB of HBM per device.

```python
import math
import jax
import jax.numpy as jnp
import numpy as np
from jax import lax

CONTRIB = 512
F = 1024
ROWS_SRC = 128
FRONTS = 8
MOST = 32
ROWS = 4096
N_FRONT = 8
N_SUB = 4


def draw_child_factors(key, part):
    key_diag = jax.random.fold_in(key, 11)
    key_off = jax.random.fold_in(key, 12)
    shape = (2 * FRONTS, CONTRIB, CONTRIB)
    diagonal = jnp.exp(jax.random.uniform(key_diag, (2 * FRONTS, CONTRIB), jnp.float32, jnp.log(0.5), jnp.log(2.0)))
    offdiag = jnp.clip(jax.random.normal(key_off, shape, jnp.float32), -5.0, 5.0) * (0.5 / jnp.sqrt(jnp.float32(CONTRIB)))
    upper_mask = jnp.triu(jnp.ones((CONTRIB, CONTRIB), jnp.float32), 1)
    eye_mask = jnp.eye(CONTRIB, dtype=jnp.float32)
    return (offdiag * upper_mask[None] + diagonal[:, :, None] * eye_mask[None]).astype(jnp.float32)


def draw_child_columns(key, part):
    key_score = jax.random.fold_in(key, 21)
    scores = jax.random.randint(key_score, (2 * FRONTS, F), 0, 2 ** 19, jnp.int32)
    distinct = scores * F + jnp.arange(F, dtype=jnp.int32)[None, :]
    permuted = jnp.argsort(distinct, axis=1, stable=True).astype(jnp.int32)
    return permuted[:, :CONTRIB]


def level_of(key, extent, cuts, low, largest):
    gain = 1.0
    for position, parts in cuts:
        steps = jax.random.uniform(jax.random.fold_in(jax.random.fold_in(key, 6), position), (parts,), jnp.float32, low / len(cuts), largest / len(cuts))
        gain = gain * jnp.repeat(jnp.exp(steps), extent[position] // parts).reshape((-1,) + (1,) * (len(extent) - 1 - position))
    return gain


def shared_out(stream_key, own, number, rows, number_of, top, reach, skew):
    order = jax.random.permutation(stream_key, number_of)
    crowded, usual = load_shares(number_of, rows * top, reach, skew, True), load_shares(number_of, rows * top, reach, skew, False)
    places = jnp.arange(number_of)

    def named(tallies, rotation):
        used = int((tallies > 0).sum())
        fixed = max(1, used // 4)
        passed = fixed + (places - fixed + rotation * (used - fixed)) % max(1, number_of - fixed)
        return jnp.zeros((number_of,), jnp.int32).at[order[jnp.where(places < fixed, places, passed)]].set(jnp.asarray(tallies, jnp.int32))

    tallies = jnp.where(number % 4 == 0, named(crowded, number // 4), named(usual, number - number // 4 - 1))
    mixed = jax.random.permutation(jax.random.fold_in(own, 3), number_of)
    giver, taker = mixed[0:number_of // 2 * 2:2], mixed[1:number_of // 2 * 2:2]
    slack = jnp.minimum(tallies[giver] - 1, reach - tallies[taker]) // 2
    slack = jnp.where((giver == order[0]) | (taker == order[0]) | (tallies[taker] == 0), 0, jnp.maximum(slack, 0))
    passed = jax.random.randint(jax.random.fold_in(own, 4), (number_of // 2,), 0, 1 << 20) % (slack + 1)
    tallies = tallies.at[giver].add(-passed).at[taker].add(passed)
    items = jnp.searchsorted(jnp.cumsum(tallies), jnp.arange(rows * top), side="right").astype(jnp.int32)
    listing = items.reshape(top, rows).T
    listing = listing[jax.random.permutation(jax.random.fold_in(own, 1), rows)]
    rotation = jax.random.randint(jax.random.fold_in(own, 2), (rows, 1), 0, top)
    return jnp.take_along_axis(listing, (jnp.arange(top)[None, :] + rotation) % top, axis=1)


def load_shares(number_of, total, limit, slope, full):
    portions = [(1 << 20) // math.isqrt(rank ** slope) + 1 for rank in range(1, number_of + 1)]
    largest = limit if full else min(limit, max(-(-total // number_of), total * portions[0] // sum(portions)))
    least = 1 if total - largest >= number_of - 1 else 0
    holding, spare = [largest] + [least] * (number_of - 1), total - largest - least * (number_of - 1)
    while spare > 0:
        free = [i for i in range(1, number_of) if holding[i] < largest] or [i for i in range(1, number_of) if holding[i] < limit]
        pool, remaining = sum([portions[i] for i in free]), spare
        for i in free:
            addition = min(limit - holding[i], max(1, remaining * portions[i] // pool), spare)
            holding[i] = holding[i] + addition
            spare = spare - addition
    return np.array(holding)


def noise(rng, extent, scale, limit, pieces=(), held_as=jnp.bfloat16):
    level = level_of(rng, extent, pieces, -0.22, 0.18) if pieces else 1.0
    values = jax.random.normal(rng, extent, jnp.float32) * scale * level
    return jnp.minimum(jnp.maximum(values, -limit), limit).astype(held_as)


def setup_inputs(seed: int = 0) -> dict:
    key_list = jax.random.split(jax.random.key(seed), 6)
    row_values = noise(key_list[0], (ROWS, F), 0.02, 0.12, ((0, 32),), jnp.float32)
    front_of_row_keys = jax.random.split(jax.random.fold_in(key_list[1], 1), ROWS // ROWS_SRC)
    front_of_row_turns = jax.random.permutation(jax.random.fold_in(key_list[1], 3), ROWS // ROWS_SRC)
    front_of_row = jax.vmap(lambda own, number: shared_out(jax.random.fold_in(key_list[1], 2), own, number, ROWS_SRC, FRONTS, 1, MOST, 2))(front_of_row_keys, front_of_row_turns).reshape((ROWS, 1))
    child_factors = draw_child_factors(jax.random.fold_in(key_list[5], 71), 0)
    child_columns = draw_child_columns(jax.random.fold_in(key_list[5], 71), 0)
    damping = jnp.clip(jnp.exp(math.log(2.0) - 1.3862944 * jax.random.uniform(key_list[4], (FRONTS, F), jnp.float32) ** level_of(key_list[4], (FRONTS, F), ((0, 8),), -0.2, 0.2)), 0.5, 2.0)
    return {"row_values": row_values, "front_of_row": front_of_row, "child_factors": child_factors, "child_columns": child_columns, "damping": damping}


HIGHEST = lax.Precision.HIGHEST

def gram_product(matrix):
    return lax.dot_general(matrix.astype(jnp.float32), matrix.astype(jnp.float32), (((0,), (0,)), ((), ())), precision=HIGHEST, preferred_element_type=jnp.float32)

def reference(row_values, front_of_row, child_factors, child_columns, damping):
    destination = front_of_row[:, 0].astype(jnp.int32)
    sorted_rows = jnp.argsort(destination, stable=True).astype(jnp.int32)
    counts = jnp.bincount(destination, length=FRONTS).astype(jnp.int32)
    starts = (jnp.cumsum(counts) - counts).astype(jnp.int32)
    capacity = MOST * N_FRONT * N_SUB
    padded_order = jnp.concatenate([sorted_rows, jnp.zeros((capacity,), jnp.int32)])
    columns = jnp.arange(F, dtype=jnp.int32)

    def factor_front(front_index):
        row_index = lax.dynamic_slice(padded_order, (starts[front_index],), (capacity,))
        is_live = jnp.arange(capacity, dtype=jnp.int32) < counts[front_index]
        front_rows = jnp.where(is_live[:, None], row_values[row_index], jnp.float32(0.0))
        gram_matrix = gram_product(front_rows)
        for child_index in range(2):
            child = child_factors[2 * front_index + child_index]
            mapping = child_columns[2 * front_index + child_index]
            spread = (mapping[:, None] == columns[None, :]).astype(jnp.float32)
            placed = jnp.dot(child.astype(jnp.float32), spread.astype(jnp.float32), precision=HIGHEST, preferred_element_type=jnp.float32)
            gram_matrix = gram_matrix + gram_product(placed)
        weight = damping[front_index]
        gram_matrix = gram_matrix + jnp.diag(weight * weight)
        return jnp.linalg.cholesky(gram_matrix).T
    return lax.map(factor_front, jnp.arange(FRONTS, dtype=jnp.int32))
```

```python
import jax, jax.numpy as jnp
from jax import lax
from jax.experimental import pallas as pl
from jax.experimental.pallas import tpu as pltpu
from jax.sharding import PartitionSpec as P

HIGHEST = lax.Precision.HIGHEST

NB = 128
BF = jnp.bfloat16
F32 = jnp.float32


def split3(x):
    h = x.astype(BF)
    r = x - h.astype(F32)
    m = r.astype(BF)
    l = (r - m.astype(F32)).astype(BF)
    return h, m, l


def split2(x):
    h = x.astype(BF)
    return h, (x - h.astype(F32)).astype(BF)


def tdot(a, b):
    return lax.dot_general(a, b, (((0,), (0,)), ((), ())), preferred_element_type=F32)


def mm(a, b):
    return lax.dot_general(a, b, (((1,), (0,)), ((), ())), preferred_element_type=F32)


def factor_diag(m_ref, B):
    for b in range(NB // B):
        lo = b * B
        rows = m_ref[lo:lo + B, :]
        sub = lax.broadcasted_iota(jnp.int32, (B, 1), 0)
        cs = [jnp.broadcast_to(rows[:, lo + j:lo + j + 1], (B, NB)) for j in range(B)]
        for j in range(B):
            c = cs[j]
            r = lax.rsqrt(c[j:j + 1, :])
            mult = jnp.where(sub > j, c * r, 0.0)
            r2 = jnp.concatenate([r, r], axis=1)
            pivot = rows[j:j + 1, :] * r2
            m2 = jnp.concatenate([mult, mult], axis=1)
            rows = jnp.where(sub == j, pivot, rows - m2 * pivot)
            for i in range(j + 1, B):
                cs[i] = cs[i] - mult * (cs[i][j:j + 1, :] * r)
        m_ref[lo:lo + B, :] = rows
        if lo + B < NB:
            h, m, l = split3(rows)
            left = jnp.concatenate([h, h, m, h, l, m], axis=0)[:, :NB]
            right = jnp.concatenate([h, m, h, l, h, m], axis=0)
            upd = tdot(left, right)
            m_ref[lo + B:, :] = m_ref[lo + B:, :] - upd[lo + B:, :]


def chol_body(own, per, B, g_ref, o_ref, a_ref, m_ref, rl_ref, rr_ref):
    F = g_ref.shape[0]
    panels = F // NB
    a_ref[...] = g_ref[...]
    ri = lax.broadcasted_iota(jnp.int32, (NB, NB), 0)
    ci = lax.broadcasted_iota(jnp.int32, (NB, NB), 1)

    def panel(p, carry):
        p0 = pl.multiple_of(p * NB, NB)
        m_ref[:, :NB] = a_ref[pl.ds(p0, NB), pl.ds(p0, NB)]
        m_ref[:, NB:] = (ri == ci).astype(F32)
        factor_diag(m_ref, B)
        th, tl = split2(jnp.where(ci <= ri, m_ref[:, NB:], 0.0))
        tcat = jnp.concatenate([th, th, tl], axis=1)

        def cols(j, c):
            j0 = pl.multiple_of(j * NB, NB)
            h, l = split2(a_ref[pl.ds(p0, NB), pl.ds(j0, NB)])
            r = mm(tcat, jnp.concatenate([h, l, h], axis=0))
            a_ref[pl.ds(p0, NB), pl.ds(j0, NB)] = r
            h, l = split2(r)
            rl_ref[:, pl.ds(j0, NB)] = jnp.concatenate([h, h, l], axis=0)
            rr_ref[:, pl.ds(j0, NB)] = jnp.concatenate([h, l, h], axis=0)
            return c

        lax.fori_loop(p + 1, panels, cols, 0)
        a_ref[pl.ds(p0, NB), pl.ds(p0, NB)] = jnp.where(ci >= ri, m_ref[:, :NB], 0.0)

        @pl.when(p // per == own)
        def _():
            off = pl.multiple_of((p - own * per) * NB, NB)
            def put(j, c):
                j0 = pl.multiple_of(j * NB, NB)
                v = a_ref[pl.ds(p0, NB), pl.ds(j0, NB)]
                o_ref[pl.ds(off, NB), pl.ds(j0, NB)] = jnp.where(j >= p, v, 0.0)
                return c
            lax.fori_loop(0, panels, put, 0)

        def trail(i, c):
            i0 = pl.multiple_of(i * NB, NB)
            lt = rl_ref[:, pl.ds(i0, NB)].T

            def inner(j, cc):
                j0 = pl.multiple_of(j * NB, NB)
                a_ref[pl.ds(i0, NB), pl.ds(j0, NB)] -= mm(lt, rr_ref[:, pl.ds(j0, NB)])
                return cc

            lax.fori_loop(i, panels, inner, 0)
            return c

        lax.fori_loop(p + 1, panels, trail, 0)
        return carry

    lax.fori_loop(0, (own + 1) * per, panel, 0)


def chol(g, subs, B=16):
    F = g.shape[0]
    rows = F // subs

    def body(g_ref, o_ref, *scratch):
        chol_body(lax.axis_index("sub"), rows // NB, B, g_ref, o_ref, *scratch)

    return pl.pallas_call(
        body,
        out_shape=jax.ShapeDtypeStruct((rows, F), F32),
        in_specs=[pl.BlockSpec(memory_space=pltpu.VMEM)],
        out_specs=pl.BlockSpec(memory_space=pltpu.VMEM),
        scratch_shapes=[
            pltpu.VMEM((F, F), F32),
            pltpu.VMEM((NB, 2 * NB), F32),
            pltpu.VMEM((3 * NB, F), BF),
            pltpu.VMEM((3 * NB, F), BF),
        ],
        compiler_params=pltpu.CompilerParams(vmem_limit_bytes=40 << 20),
        name="chol",
    )(g)


def cross_product(left_cols, right_cols):
    return lax.dot_general(
        left_cols,
        right_cols,
        (((0,), (0,)), ((), ())),
        precision=HIGHEST,
        preferred_element_type=jnp.float32,
    )


def local(row_values, front_of_row, child_factors, child_columns, damping):
    fronts = lax.axis_size("front")
    rows_held, front_width = row_values.shape
    capacity = 2 * rows_held // fronts
    destination = front_of_row[:, 0]
    onehot = (destination[:, None] == jnp.arange(fronts, dtype=jnp.int32)[None, :]).astype(
        jnp.int32
    )
    position = jnp.sum((jnp.cumsum(onehot, axis=0) - onehot) * onehot, axis=1)
    slot_of = destination * capacity + position
    source = (
        jnp.full((fronts * capacity,), rows_held, jnp.int32)
        .at[slot_of]
        .set(jnp.arange(rows_held, dtype=jnp.int32))
    )
    padded = jnp.concatenate([row_values, jnp.zeros((1, front_width), row_values.dtype)], axis=0)
    outgoing = padded[source]
    received = lax.all_to_all(outgoing, "front", split_axis=0, concat_axis=0, tiled=True)
    columns = jnp.arange(front_width, dtype=jnp.int32)
    spread = (child_columns[:, :, None] == columns[None, None, :]).astype(jnp.float32)
    placed = jnp.einsum(
        "jrc,jcf->jrf", child_factors, spread, precision=HIGHEST, preferred_element_type=jnp.float32
    )
    stacked = jnp.concatenate([placed.reshape(-1, front_width), received], axis=0)
    sub_count = lax.axis_size("sub")
    weight = damping[0]
    summed_gram = lax.psum(cross_product(stacked, stacked), "sub")
    summed_gram = summed_gram + jnp.diag(weight * weight)
    return chol(summed_gram, sub_count)[None]


def solution(mesh):
    in_specs = (
        P(("front", "sub"), None),
        P(("front", "sub"), None),
        P("front", "sub", None),
        P("front", None),
        P("front", None),
    )
    out_specs = P("front", "sub", None)
    return jax.shard_map(local, mesh=mesh, in_specs=in_specs, out_specs=out_specs, check_vma=False)
```

```python
import functools
import jax, jax.numpy as jnp
from jax import lax
from jax.experimental import pallas as pl
from jax.experimental.pallas import tpu as pltpu
from jax.sharding import PartitionSpec as P

HIGHEST = lax.Precision.HIGHEST

NB = 128
LAG = 3
BF = jnp.bfloat16
F32 = jnp.float32


def split3(x):
    h = x.astype(BF)
    r = x - h.astype(F32)
    m = r.astype(BF)
    l = (r - m.astype(F32)).astype(BF)
    return h, m, l


def split2(x):
    h = x.astype(BF)
    return h, (x - h.astype(F32)).astype(BF)


def tdot(a, b):
    return lax.dot_general(a, b, (((0,), (0,)), ((), ())), preferred_element_type=F32)


def mm(a, b):
    return lax.dot_general(a, b, (((1,), (0,)), ((), ())), preferred_element_type=F32)


def factor_diag(m_ref, B, slot):
    for b in range(NB // B):
        lo = b * B
        slot(b)
        rows = m_ref[lo:lo + B, :]
        sub = lax.broadcasted_iota(jnp.int32, (B, 1), 0)
        cs = [jnp.broadcast_to(rows[:, lo + j:lo + j + 1], (B, NB)) for j in range(B)]
        for j in range(B):
            c = cs[j]
            r = lax.rsqrt(c[j:j + 1, :])
            mult = jnp.where(sub > j, c * r, 0.0)
            r2 = jnp.concatenate([r, r], axis=1)
            pivot = rows[j:j + 1, :] * r2
            m2 = jnp.concatenate([mult, mult], axis=1)
            rows = jnp.where(sub == j, pivot, rows - m2 * pivot)
            for i in range(j + 1, B):
                cs[i] = cs[i] - mult * (cs[i][j:j + 1, :] * r)
        m_ref[lo:lo + B, :] = rows
        if lo + B < NB:
            h, m, l = split3(rows)
            left = jnp.concatenate([h, h, m, h, l, m], axis=0)[:, :NB]
            right = jnp.concatenate([h, m, h, l, h, m], axis=0)
            upd = tdot(left, right)
            m_ref[lo + B:, :] = m_ref[lo + B:, :] - upd[lo + B:, :]


MESH = pl.DeviceIdType.MESH


def fused_body(n, B, x_ref, w_ref, o_ref, a_ref, m_ref, rl_ref, rr_ref, xl_ref, xr_ref, p_ref, l_ref, r_ref, fr_ref, fl_ref, sr, sl, gl, gr):
    K, F = x_ref.shape
    panels = F // NB
    per = panels // n
    me = lax.axis_index("sub")
    right, left = lax.rem(me + 1, n), lax.rem(me + n - 1, n)
    first, last = me == 0, me == n - 1

    barrier = pltpu.get_barrier_semaphore()
    for peer in (left, right):
        pl.semaphore_signal(barrier, inc=1, device_id={"sub": peer}, device_id_type=MESH)
    pl.semaphore_wait(barrier, 2)

    ri = lax.broadcasted_iota(jnp.int32, (NB, NB), 0)
    ci = lax.broadcasted_iota(jnp.int32, (NB, NB), 1)

    def at(i, j):
        return (pl.ds(pl.multiple_of(i * NB, NB), NB), pl.ds(pl.multiple_of(j * NB, NB), NB))

    total = panels * (panels + 1) // 2
    ahead_left, ahead_right = LAG * (n - 1 - me), LAG * me

    def place(i, j):
        return i * panels - i * (i - 1) // 2 + j - i

    def to_right(src, c):
        return pltpu.make_async_remote_copy(
            src_ref=src.at[c], dst_ref=l_ref.at[c], send_sem=sr.at[c], recv_sem=gl.at[c],
            device_id={"sub": right}, device_id_type=MESH)

    def to_left(src, c):
        return pltpu.make_async_remote_copy(
            src_ref=src.at[c], dst_ref=r_ref.at[c], send_sem=sl.at[c], recv_sem=gr.at[c],
            device_id={"sub": left}, device_id_type=MESH)

    h, l = split2(x_ref[...])
    xr_ref[...] = jnp.concatenate([h, l, h], axis=0)
    xl_ref[...] = jnp.concatenate([h, h, l], axis=0)

    def gram_row(i, carry):
        lt = xl_ref[:, pl.ds(pl.multiple_of(i * NB, NB), NB)].T

        def gram_col(j, c):
            c0 = place(i, j)
            p_ref[c0] = mm(lt, xr_ref[:, pl.ds(pl.multiple_of(j * NB, NB), NB)])

            @pl.when(first)
            def _():
                to_right(p_ref, c0).start()

            @pl.when(last)
            def _():
                to_left(p_ref, c0).start()
            return c

        return lax.fori_loop(i, panels, gram_col, carry)

    lax.fori_loop(0, panels, gram_row, 0)

    def from_left(c):
        @pl.when((me > 0) & (c >= 0) & (c < total))
        def _():
            to_right(fr_ref, c).wait_recv()

            @pl.when(me < n - 1)
            def _():
                fr_ref[c] = l_ref[c] + p_ref[c]
                to_right(fr_ref, c).start()

    def from_right(c):
        @pl.when((me < n - 1) & (c >= 0) & (c < total))
        def _():
            to_left(fl_ref, c).wait_recv()

            @pl.when(me > 0)
            def _():
                fl_ref[c] = r_ref[c] + p_ref[c]
                to_left(fl_ref, c).start()

    def pass_on(q):
        from_left(q + ahead_left)
        from_right(q + ahead_right)

    def serve(i, j):
        c = place(i, j)
        pass_on(c)

        @pl.when(first)
        def _():
            a_ref[at(i, j)] = p_ref[c] + r_ref[c]

        @pl.when(last)
        def _():
            a_ref[at(i, j)] = p_ref[c] + l_ref[c]

        @pl.when((me > 0) & (me < n - 1))
        def _():
            a_ref[at(i, j)] = fr_ref[c] + r_ref[c]

        @pl.when(i == j)
        def _():
            wt = w_ref[:, pl.ds(pl.multiple_of(i * NB, NB), NB)]
            a_ref[at(i, j)] += jnp.where(ri == ci, wt * wt, 0.0)

    def fill(t, c):
        pass_on(t - LAG * (n - 1))
        return c

    lax.fori_loop(0, LAG * (n - 1), fill, 0)

    def first_row(j, c):
        serve(0, j)
        return c

    lax.fori_loop(0, panels, first_row, 0)

    def panel(p, carry):
        m_ref[:, :NB] = a_ref[at(p, p)]
        m_ref[:, NB:] = (ri == ci).astype(F32)

        def slot(k):
            @pl.when(p + 1 + k < panels)
            def _():
                serve(p + 1, p + 1 + k)

        factor_diag(m_ref, B, slot)

        def rest(k, c):
            @pl.when(p + 1 + k < panels)
            def _():
                serve(p + 1, p + 1 + k)
            return c

        lax.fori_loop(NB // B, max(NB // B, panels - 1), rest, 0)
        th, tl = split2(jnp.where(ci <= ri, m_ref[:, NB:], 0.0))
        tcat = jnp.concatenate([th, th, tl], axis=1)

        def cols(j, c):
            j0 = pl.multiple_of(j * NB, NB)
            h, l = split2(a_ref[at(p, j)])
            r = mm(tcat, jnp.concatenate([h, l, h], axis=0))
            a_ref[at(p, j)] = r
            h, l = split2(r)
            rl_ref[p, :, pl.ds(j0, NB)] = jnp.concatenate([h, h, l], axis=0)
            rr_ref[p, :, pl.ds(j0, NB)] = jnp.concatenate([h, l, h], axis=0)
            return c

        lax.fori_loop(p + 1, panels, cols, 0)
        a_ref[at(p, p)] = jnp.where(ci >= ri, m_ref[:, :NB], 0.0)

        @pl.when(p // per == me)
        def _():
            off = p - me * per

            def put(j, c):
                o_ref[at(off, j)] = jnp.where(j >= p, a_ref[at(p, j)], 0.0)
                return c
            lax.fori_loop(0, panels, put, 0)

        @pl.when(p + 1 < panels)
        def _():
            def term(q, c):
                lt = rl_ref[q, :, pl.ds(pl.multiple_of((p + 1) * NB, NB), NB)].T

                def inner(j, cc):
                    a_ref[at(p + 1, j)] -= mm(lt, rr_ref[q, :, pl.ds(pl.multiple_of(j * NB, NB), NB)])
                    return cc
                return lax.fori_loop(p + 1, panels, inner, c)
            lax.fori_loop(0, p + 1, term, 0)
        return carry

    lax.fori_loop(0, panels, panel, 0)

    def drain(c, carry):
        @pl.when(me < n - 1)
        def _():
            to_right(fr_ref, c).wait_send()

        @pl.when(me > 0)
        def _():
            to_left(fl_ref, c).wait_send()
        return carry

    lax.fori_loop(0, total, drain, 0)


def merge(x, w, n, B=16):
    K, F = x.shape
    panels = F // NB
    total = panels * (panels + 1) // 2
    sems = pltpu.SemaphoreType.DMA((total,))
    return pl.pallas_call(
        functools.partial(fused_body, n, B),
        out_shape=jax.ShapeDtypeStruct((F // n, F), F32),
        in_specs=[pl.BlockSpec(memory_space=pltpu.VMEM)] * 2,
        out_specs=pl.BlockSpec(memory_space=pltpu.VMEM),
        scratch_shapes=[
            pltpu.VMEM((F, F), F32),
            pltpu.VMEM((NB, 2 * NB), F32),
            pltpu.VMEM((panels, 3 * NB, F), BF),
            pltpu.VMEM((panels, 3 * NB, F), BF),
            pltpu.VMEM((3 * K, F), BF),
            pltpu.VMEM((3 * K, F), BF),
        ] + [pltpu.VMEM((total, NB, NB), F32)] * 5 + [sems] * 4,
        compiler_params=pltpu.CompilerParams(
            vmem_limit_bytes=60 << 20, collective_id=0, has_side_effects=True),
        name="merge",
    )(x, w)


def local(row_values, front_of_row, child_factors, child_columns, damping):
    fronts = lax.axis_size("front")
    rows_held, front_width = row_values.shape
    capacity = 2 * rows_held // fronts
    destination = front_of_row[:, 0]
    onehot = (destination[:, None] == jnp.arange(fronts, dtype=jnp.int32)[None, :]).astype(
        jnp.int32
    )
    position = jnp.sum((jnp.cumsum(onehot, axis=0) - onehot) * onehot, axis=1)
    slot_of = destination * capacity + position
    source = (
        jnp.full((fronts * capacity,), rows_held, jnp.int32)
        .at[slot_of]
        .set(jnp.arange(rows_held, dtype=jnp.int32))
    )
    padded = jnp.concatenate([row_values, jnp.zeros((1, front_width), row_values.dtype)], axis=0)
    outgoing = padded[source]
    received = lax.all_to_all(outgoing, "front", split_axis=0, concat_axis=0, tiled=True)
    columns = jnp.arange(front_width, dtype=jnp.int32)
    spread = (child_columns[:, :, None] == columns[None, None, :]).astype(jnp.float32)
    placed = jnp.einsum(
        "jrc,jcf->jrf", child_factors, spread, precision=HIGHEST, preferred_element_type=jnp.float32
    )
    stacked = jnp.concatenate([placed.reshape(-1, front_width), received], axis=0)
    sub_count = lax.axis_size("sub")
    return merge(stacked, damping, sub_count)[None]


def solution(mesh):
    in_specs = (
        P(("front", "sub"), None),
        P(("front", "sub"), None),
        P("front", "sub", None),
        P("front", None),
        P("front", None),
    )
    out_specs = P("front", "sub", None)
    return jax.shard_map(local, mesh=mesh, in_specs=in_specs, out_specs=out_specs, check_vma=False)
```

```python
import functools
import jax, jax.numpy as jnp
from jax import lax
from jax.experimental import pallas as pl
from jax.experimental.pallas import tpu as pltpu
from jax.sharding import PartitionSpec as P

NB = 128
LAG = 3
BF = jnp.bfloat16
F32 = jnp.float32


def split3(x):
    h = x.astype(BF)
    r = x - h.astype(F32)
    m = r.astype(BF)
    l = (r - m.astype(F32)).astype(BF)
    return h, m, l


def split2(x):
    h = x.astype(BF)
    return h, (x - h.astype(F32)).astype(BF)


def tdot(a, b):
    return lax.dot_general(a, b, (((0,), (0,)), ((), ())), preferred_element_type=F32)


def mm(a, b):
    return lax.dot_general(a, b, (((1,), (0,)), ((), ())), preferred_element_type=F32)


def factor_diag(m_ref, B, slot):
    for b in range(NB // B):
        lo = b * B
        slot(b)
        rows = m_ref[lo:lo + B, :]
        sub = lax.broadcasted_iota(jnp.int32, (B, 1), 0)
        cs = [jnp.broadcast_to(rows[:, lo + j:lo + j + 1], (B, NB)) for j in range(B)]
        for j in range(B):
            c = cs[j]
            r = lax.rsqrt(c[j:j + 1, :])
            mult = jnp.where(sub > j, c * r, 0.0)
            r2 = jnp.concatenate([r, r], axis=1)
            pivot = rows[j:j + 1, :] * r2
            m2 = jnp.concatenate([mult, mult], axis=1)
            rows = jnp.where(sub == j, pivot, rows - m2 * pivot)
            for i in range(j + 1, B):
                cs[i] = cs[i] - mult * (cs[i][j:j + 1, :] * r)
        m_ref[lo:lo + B, :] = rows
        if lo + B < NB:
            h, m, l = split3(rows)
            left = jnp.concatenate([h, h, m, h, l, m], axis=0)[:, :NB]
            right = jnp.concatenate([h, m, h, l, h, m], axis=0)
            upd = tdot(left, right)
            m_ref[lo + B:, :] = m_ref[lo + B:, :] - upd[lo + B:, :]


MESH = pl.DeviceIdType.MESH


def fused_body(n, fronts, cap, B, x_ref, d_ref, ch_ref, cc_ref, w_ref, o_ref, out_ref, in_ref, fs, fg, a_ref, m_ref, rl_ref, rr_ref, xl_ref, xr_ref, p_ref, l_ref, r_ref, fr_ref, fl_ref, sr, sl, gl, gr):
    R, F = x_ref.shape
    kids, crows, _ = ch_ref.shape
    slots = fronts * cap
    K = kids * crows + slots
    panels = F // NB
    per = panels // n
    me = lax.axis_index("sub")
    right, left = lax.rem(me + 1, n), lax.rem(me + n - 1, n)
    first, last = me == 0, me == n - 1

    mine = lax.axis_index("front")
    barrier = pltpu.get_barrier_semaphore()
    for peer in (left, right):
        pl.semaphore_signal(barrier, inc=1, device_id={"sub": peer}, device_id_type=MESH)

    def greet(k, c):
        pl.semaphore_signal(barrier, inc=1, device_id={"front": lax.rem(mine + k, fronts)}, device_id_type=MESH)
        return c

    lax.fori_loop(1, fronts, greet, 0)

    dest = d_ref[...]
    hot = dest == lax.broadcasted_iota(jnp.int32, (R, fronts), 1)
    below = lax.broadcasted_iota(jnp.int32, (R, R), 1) < lax.broadcasted_iota(jnp.int32, (R, R), 0)
    before = mm(below.astype(F32).astype(BF), hot.astype(F32).astype(BF))
    position = jnp.sum(jnp.where(hot, before, 0.0), axis=1, keepdims=True)
    slot_of = dest.astype(F32) * cap + position
    pick = (slot_of == lax.broadcasted_iota(jnp.int32, (R, slots), 1).astype(F32)).astype(F32).astype(BF)
    out_ref[...] = tdot(jnp.concatenate([pick] * 3, axis=0), jnp.concatenate(split3(x_ref[...]), axis=0))
    pl.semaphore_wait(barrier, fronts + 1)

    def rows_of(f):
        return pl.ds(pl.multiple_of(f * cap, cap), cap)

    def post(k, dst_front):
        to = lax.rem(mine + k, fronts)
        return pltpu.make_async_remote_copy(
            src_ref=out_ref.at[rows_of(to)], dst_ref=in_ref.at[rows_of(dst_front)], send_sem=fs.at[k],
            recv_sem=fg.at[k], device_id={"front": to}, device_id_type=MESH)

    def post_rows(k, c):
        post(k, mine).start()
        return c

    lax.fori_loop(1, fronts, post_rows, 0)
    in_ref[rows_of(mine), :] = out_ref[rows_of(mine), :]

    def keep(start, count, h, l):
        for ref, parts in ((xr_ref, (h, l, h)), (xl_ref, (h, h, l))):
            for t, part in enumerate(parts):
                ref[t * K + start:t * K + start + count, :] = part

    for kid in range(kids):
        h, l = split2(ch_ref[kid])
        spread = (lax.broadcasted_iota(jnp.int32, (F, cc_ref.shape[1]), 0) == cc_ref[kid:kid + 1, :]).astype(F32).astype(BF)
        both = lax.dot_general(jnp.concatenate([h, l], axis=0), spread, (((1,), (1,)), ((), ())), preferred_element_type=F32)
        keep(kid * crows, crows, both[:crows].astype(BF), both[crows:].astype(BF))

    def take(k, c):
        post(k, lax.rem(mine + fronts - k, fronts)).wait_recv()
        return c

    lax.fori_loop(1, fronts, take, 0)
    h, l = split2(in_ref[...])
    keep(kids * crows, slots, h, l)

    ri = lax.broadcasted_iota(jnp.int32, (NB, NB), 0)
    ci = lax.broadcasted_iota(jnp.int32, (NB, NB), 1)

    def at(i, j):
        return (pl.ds(pl.multiple_of(i * NB, NB), NB), pl.ds(pl.multiple_of(j * NB, NB), NB))

    total = panels * (panels + 1) // 2
    ahead_left, ahead_right = LAG * (n - 1 - me), LAG * me

    def place(i, j):
        return i * panels - i * (i - 1) // 2 + j - i

    def to_right(src, c):
        return pltpu.make_async_remote_copy(
            src_ref=src.at[c], dst_ref=l_ref.at[c], send_sem=sr.at[c], recv_sem=gl.at[c],
            device_id={"sub": right}, device_id_type=MESH)

    def to_left(src, c):
        return pltpu.make_async_remote_copy(
            src_ref=src.at[c], dst_ref=r_ref.at[c], send_sem=sl.at[c], recv_sem=gr.at[c],
            device_id={"sub": left}, device_id_type=MESH)

    WB = 2 * NB

    def gram_row(i, carry):
        lt = xl_ref[:, pl.ds(pl.multiple_of(i * WB, WB), WB)].T

        def gram_col(j, c):
            block = mm(lt, xr_ref[:, pl.ds(pl.multiple_of(j * WB, WB), WB)])
            p_ref[place(2 * i, 2 * j)] = block[:NB, :NB]
            p_ref[place(2 * i, 2 * j + 1)] = block[:NB, NB:]
            p_ref[place(2 * i + 1, 2 * j + 1)] = block[NB:, NB:]

            @pl.when(j > i)
            def _():
                p_ref[place(2 * i + 1, 2 * j)] = block[NB:, :NB]
            return c

        lax.fori_loop(i, panels // 2, gram_col, 0)

        def launch(c, cc):
            @pl.when(first)
            def _():
                to_right(p_ref, c).start()

            @pl.when(last)
            def _():
                to_left(p_ref, c).start()
            return cc

        return lax.fori_loop(place(2 * i, 2 * i), place(2 * i + 2, 2 * i + 2), launch, carry)

    lax.fori_loop(0, panels // 2, gram_row, 0)

    def from_left(c):
        @pl.when((me > 0) & (c >= 0) & (c < total))
        def _():
            to_right(fr_ref, c).wait_recv()

            @pl.when(me < n - 1)
            def _():
                fr_ref[c] = l_ref[c] + p_ref[c]
                to_right(fr_ref, c).start()

    def from_right(c):
        @pl.when((me < n - 1) & (c >= 0) & (c < total))
        def _():
            to_left(fl_ref, c).wait_recv()

            @pl.when(me > 0)
            def _():
                fl_ref[c] = r_ref[c] + p_ref[c]
                to_left(fl_ref, c).start()

    def pass_on(q):
        from_left(q + ahead_left)
        from_right(q + ahead_right)

    def serve(i, j):
        c = place(i, j)
        pass_on(c)

        @pl.when(first)
        def _():
            a_ref[at(i, j)] = p_ref[c] + r_ref[c]

        @pl.when(last)
        def _():
            a_ref[at(i, j)] = p_ref[c] + l_ref[c]

        @pl.when((me > 0) & (me < n - 1))
        def _():
            a_ref[at(i, j)] = fr_ref[c] + r_ref[c]

        @pl.when(i == j)
        def _():
            wt = w_ref[:, pl.ds(pl.multiple_of(i * NB, NB), NB)]
            a_ref[at(i, j)] += jnp.where(ri == ci, wt * wt, 0.0)

    def fill(t, c):
        pass_on(t - LAG * (n - 1))
        return c

    lax.fori_loop(0, LAG * (n - 1), fill, 0)

    def first_row(j, c):
        serve(0, j)
        return c

    lax.fori_loop(0, panels, first_row, 0)

    def panel(p, carry):
        m_ref[:, :NB] = a_ref[at(p, p)]
        m_ref[:, NB:] = (ri == ci).astype(F32)

        def slot(k):
            @pl.when(p + 1 + k < panels)
            def _():
                serve(p + 1, p + 1 + k)

        factor_diag(m_ref, B, slot)

        def rest(k, c):
            @pl.when(p + 1 + k < panels)
            def _():
                serve(p + 1, p + 1 + k)
            return c

        lax.fori_loop(NB // B, max(NB // B, panels - 1), rest, 0)
        th, tl = split2(jnp.where(ci <= ri, m_ref[:, NB:], 0.0))
        tcat = jnp.concatenate([th, th, tl], axis=1)

        def cols(j, c):
            j0 = pl.multiple_of(j * NB, NB)
            h, l = split2(a_ref[at(p, j)])
            r = mm(tcat, jnp.concatenate([h, l, h], axis=0))
            a_ref[at(p, j)] = r
            h, l = split2(r)
            rl_ref[p, :, pl.ds(j0, NB)] = jnp.concatenate([h, h, l], axis=0)
            rr_ref[p, :, pl.ds(j0, NB)] = jnp.concatenate([h, l, h], axis=0)
            return c

        lax.fori_loop(p + 1, panels, cols, 0)
        a_ref[at(p, p)] = jnp.where(ci >= ri, m_ref[:, :NB], 0.0)

        @pl.when(p // per == me)
        def _():
            off = p - me * per

            def put(j, c):
                o_ref[at(off, j)] = jnp.where(j >= p, a_ref[at(p, j)], 0.0)
                return c
            lax.fori_loop(0, panels, put, 0)

        @pl.when(p + 1 < panels)
        def _():
            def term(q, c):
                lt = rl_ref[q, :, pl.ds(pl.multiple_of((p + 1) * NB, NB), NB)].T

                def inner(j, cc):
                    a_ref[at(p + 1, j)] -= mm(lt, rr_ref[q, :, pl.ds(pl.multiple_of(j * NB, NB), NB)])
                    return cc
                return lax.fori_loop(p + 1, panels, inner, c)
            lax.fori_loop(0, p + 1, term, 0)
        return carry

    lax.fori_loop(0, panels, panel, 0)

    def drain(c, carry):
        @pl.when(me < n - 1)
        def _():
            to_right(fr_ref, c).wait_send()

        @pl.when(me > 0)
        def _():
            to_left(fl_ref, c).wait_send()
        return carry

    lax.fori_loop(0, total, drain, 0)

    def sent(k, c):
        post(k, mine).wait_send()
        return c

    lax.fori_loop(1, fronts, sent, 0)


def local(row_values, front_of_row, child_factors, child_columns, damping, B=16):
    fronts, n = lax.axis_size("front"), lax.axis_size("sub")
    rows_held, F = row_values.shape
    cap = -(-(2 * rows_held // fronts) // 8) * 8
    K = fronts * cap + child_factors.shape[0] * child_factors.shape[1]
    panels = F // NB
    total = panels * (panels + 1) // 2
    sems = pltpu.SemaphoreType.DMA((total,))
    return pl.pallas_call(
        functools.partial(fused_body, n, fronts, cap, B),
        out_shape=jax.ShapeDtypeStruct((F // n, F), F32),
        in_specs=[pl.BlockSpec(memory_space=pltpu.VMEM)] * 5,
        out_specs=pl.BlockSpec(memory_space=pltpu.VMEM),
        scratch_shapes=[
            pltpu.VMEM((fronts * cap, F), F32),
            pltpu.VMEM((fronts * cap, F), F32),
            pltpu.SemaphoreType.DMA((fronts,)),
            pltpu.SemaphoreType.DMA((fronts,)),
            pltpu.VMEM((F, F), F32),
            pltpu.VMEM((NB, 2 * NB), F32),
            pltpu.VMEM((panels, 3 * NB, F), BF),
            pltpu.VMEM((panels, 3 * NB, F), BF),
            pltpu.VMEM((3 * K, F), BF),
            pltpu.VMEM((3 * K, F), BF),
        ] + [pltpu.VMEM((total, NB, NB), F32)] * 5 + [sems] * 4,
        compiler_params=pltpu.CompilerParams(
            vmem_limit_bytes=60 << 20, collective_id=0, has_side_effects=True),
        name="merge",
    )(row_values, front_of_row, child_factors, child_columns, damping)[None]


def solution(mesh):
    in_specs = (
        P(("front", "sub"), None),
        P(("front", "sub"), None),
        P("front", "sub", None),
        P("front", None),
        P("front", None),
    )
    out_specs = P("front", "sub", None)
    return jax.shard_map(local, mesh=mesh, in_specs=in_specs, out_specs=out_specs, check_vma=False)
```
